32 devices in a mesh: table: 16 (over z, y, x), row: 2 (over core).
Axes of the slice: x: 2, y: 2, z: 4, core: 2. Of those that a mesh axis runs over, the one named last changes fastest.
Arguments:
- dense_input: bfloat16 [512, 13], P(('table', 'row')), may hold values from -6 to 6
- bottom_first: bfloat16 [13, 512], replicated, may hold values from -1.75 to 1.75
- bottom_second: bfloat16 [512, 256], replicated, may hold values from -0.375 to 0.375
- bottom_third: bfloat16 [256, 128], replicated, may hold values from -0.5 to 0.5
- wide_tables: bfloat16 [131072, 256], P(('table', 'row')), may hold values from -6 to 6
- narrow_tables: bfloat16 [131072, 64], P(('table', 'row')), may hold values from -6 to 6
- wide_indices: int32 [512, 4, 8], P(('table', 'row')), may hold values from 0 to 32767
- wide_lengths: int32 [512, 4], P(('table', 'row')), may hold values from 4 to 8
- narrow_indices: int32 [512, 4, 8], P(('table', 'row')), may hold values from 0 to 32767
- narrow_lengths: int32 [512, 4], P(('table', 'row')), may hold values from 4 to 8
- wide_projection: bfloat16 [4, 256, 128], replicated, may hold values from -0.125 to 0.125
- narrow_projection: bfloat16 [4, 64, 128], replicated, may hold values from -0.25 to 0.25
- top_first: bfloat16 [164, 1024], replicated, may hold values from -0.078125 to 0.078125
- top_last: bfloat16 [1024], replicated, may hold values from -0.1875 to 0.1875
Outputs:
- hidden: bfloat16 [512, 1024], P(('table', 'row'))
- logits: float32 [512], P(('table', 'row'))
The draws below stay inside these ranges and needn't reach their ends.
All inputs are finite; a program needn't handle non-finite values.
Results may differ from the reference program's by a relative error of at most 0.02.
Values may be sent and summed in bfloat16 or wider, within the bound.
A program may use at most 64 MiB of HBM per device.

```python
import jax
import jax.numpy as jnp
import numpy as np
from jax import lax

WW = 256
WN = 64
EMB = 128
DENSE_IN = 13
BOT1 = 512
BOT2 = 256
TOP = 1024
POOL = 8
R_DEV = 4096
TW = 4
TN = 4
BATCH = 512
TABLE_ROWS = 32768
FEATURES = 9
INTER = 164


def full_choice(key, table_total, salt):
    return jax.random.randint(jax.random.fold_in(key, salt), (), 0, table_total)


def drawn_rows(key, table_total, salt):
    shard_total = TABLE_ROWS // R_DEV
    full_table = full_choice(key, table_total, salt)
    score_key = jax.random.fold_in(key, salt + 1)
    loose_key = jax.random.fold_in(key, salt + 2)
    pick_key = jax.random.fold_in(key, salt + 3)
    offset_key = jax.random.fold_in(key, salt + 4)
    scores = jax.random.randint(score_key, (BATCH, table_total, shard_total), 0, 1 << 20) * shard_total + jnp.arange(shard_total, dtype=jnp.int32)
    distinct = jnp.argsort(scores, axis=-1)[..., :POOL].astype(jnp.int32)
    loose = jax.random.randint(loose_key, (BATCH, table_total, POOL), 0, shard_total)
    scattered = jax.random.randint(pick_key, (BATCH, table_total, 1), 0, 4) == 0
    scattered = scattered & (jnp.arange(table_total)[None, :, None] != full_table)
    shards = jnp.where(scattered, loose, distinct)
    offsets = jax.random.randint(offset_key, (BATCH, table_total, POOL), 0, R_DEV)
    return (shards * R_DEV + offsets).astype(jnp.int32)


def drawn_lengths(key, table_total, salt):
    full_table = full_choice(key, table_total, salt)
    drawn = jax.random.randint(jax.random.fold_in(key, salt + 5), (BATCH, table_total), POOL // 2, POOL + 1)
    return jnp.where(jnp.arange(table_total)[None, :] == full_table, POOL, drawn).astype(jnp.int32)


def draw_wide_indices(key, part):
    return drawn_rows(key, TW, 11)


def draw_wide_lengths(key, part):
    return drawn_lengths(key, TW, 11)


def draw_narrow_indices(key, part):
    return drawn_rows(key, TN, 31)


def draw_narrow_lengths(key, part):
    return drawn_lengths(key, TN, 31)


def block_levels(own_key, extent, split, least, largest):
    level, own = 1.0, jax.random.fold_in(own_key, 6)
    for axis_at, shards_of in split:
        steps = jnp.exp(jax.random.uniform(jax.random.fold_in(own, axis_at), (shards_of,), jnp.float32, least / len(split), largest / len(split)))
        level = level * jnp.repeat(steps, extent[axis_at] // shards_of).reshape([-1 if axis == axis_at else 1 for axis in range(len(extent))])
    return level


def scatter_about(key, dims, scale, limit, cuts=(), kind=jnp.bfloat16):
    level = block_levels(key, dims, cuts, -0.22, 0.18) if cuts else 1.0
    values = jax.random.normal(key, dims, jnp.float32) * scale * level
    return jnp.minimum(jnp.maximum(values, -limit), limit).astype(kind)


def setup_inputs(seed: int = 0) -> dict:
    keys = jax.random.split(jax.random.key(seed), 15)
    dense_input = scatter_about(keys[0], (BATCH, DENSE_IN), 1.0, 6.0, ((0, 32),))
    bottom_first = scatter_about(keys[1], (DENSE_IN, BOT1), DENSE_IN ** -0.5, 1.75)
    bottom_second = scatter_about(keys[2], (BOT1, BOT2), (BOT1 // 2) ** -0.5, 0.375)
    bottom_third = scatter_about(keys[3], (BOT2, EMB), (BOT2 // 2) ** -0.5, 0.5)
    wide_tables = scatter_about(keys[4], (TW * TABLE_ROWS, WW), 1.0, 6.0, ((0, 32),))
    narrow_tables = scatter_about(keys[5], (TN * TABLE_ROWS, WN), 1.0, 6.0, ((0, 32),))
    wide_indices = draw_wide_indices(jax.random.fold_in(keys[14], 71), 0)
    wide_lengths = draw_wide_lengths(jax.random.fold_in(keys[14], 71), 0)
    narrow_indices = draw_narrow_indices(jax.random.fold_in(keys[14], 71), 0)
    narrow_lengths = draw_narrow_lengths(jax.random.fold_in(keys[14], 71), 0)
    wide_projection = scatter_about(keys[10], (TW, WW, EMB), (8 * WW) ** -0.5, 0.125)
    narrow_projection = scatter_about(keys[11], (TN, WN, EMB), (8 * WN) ** -0.5, 0.25)
    top_first = scatter_about(keys[12], (INTER, TOP), (32 * INTER) ** -0.5, 0.078125)
    top_last = scatter_about(keys[13], (TOP,), TOP ** -0.5, 0.1875)
    return {"dense_input": dense_input, "bottom_first": bottom_first, "bottom_second": bottom_second, "bottom_third": bottom_third, "wide_tables": wide_tables, "narrow_tables": narrow_tables, "wide_indices": wide_indices, "wide_lengths": wide_lengths, "narrow_indices": narrow_indices, "narrow_lengths": narrow_lengths, "wide_projection": wide_projection, "narrow_projection": narrow_projection, "top_first": top_first, "top_last": top_last}


def dense_layer(values, weight):
    return jnp.maximum(jnp.dot(values, weight, preferred_element_type=jnp.float32), 0.0).astype(jnp.bfloat16)


def pool_tables(table_rows, indices, lengths, table_total):
    tables = table_rows.reshape(table_total, table_rows.shape[0] // table_total, table_rows.shape[1])

    def one_table(operands):
        table_now, bag_ids, bag_sizes = operands
        summed = jnp.zeros((bag_ids.shape[0], table_now.shape[1]), jnp.float32)
        for slot_pos in range(bag_ids.shape[1]):
            looked_up = jnp.take(table_now, bag_ids[:, slot_pos], axis=0).astype(jnp.float32)
            summed = summed + jnp.where((bag_sizes > slot_pos)[:, None], looked_up, 0.0)
        return summed

    return lax.map(one_table, (tables, jnp.swapaxes(indices, 0, 1), jnp.swapaxes(lengths, 0, 1)))


def reference(dense_input, bottom_first, bottom_second, bottom_third, wide_tables, narrow_tables, wide_indices, wide_lengths, narrow_indices, narrow_lengths, wide_projection, narrow_projection, top_first, top_last):
    bottom = dense_layer(dense_layer(dense_layer(dense_input, bottom_first), bottom_second), bottom_third)
    wide_pooled = pool_tables(wide_tables, wide_indices, wide_lengths, TW)
    wide_embedded = jnp.einsum("tbw,twe->tbe", wide_pooled, wide_projection.astype(jnp.float32), precision=lax.Precision.HIGHEST).astype(jnp.bfloat16)
    narrow_pooled = pool_tables(narrow_tables, narrow_indices, narrow_lengths, TN).astype(jnp.bfloat16)
    narrow_embedded = jnp.einsum("tbw,twe->tbe", narrow_pooled.astype(jnp.float32), narrow_projection.astype(jnp.float32), precision=lax.Precision.HIGHEST).astype(jnp.bfloat16)
    features = jnp.concatenate([bottom[None], wide_embedded, narrow_embedded], 0).astype(jnp.float32)
    products = jnp.einsum("fbe,gbe->bfg", features, features, precision=lax.Precision.HIGHEST)
    first_side, second_side = np.triu_indices(FEATURES, 1)
    pair_values = products[:, first_side, second_side]
    joined = jnp.concatenate([bottom.astype(jnp.float32), pair_values], 1).astype(jnp.bfloat16)
    hidden = dense_layer(joined, top_first)
    logits = jnp.dot(hidden, top_last, preferred_element_type=jnp.float32)
    return hidden, logits
```

```python
import functools

import jax
import jax.numpy as jnp
from jax import lax
from jax.experimental import pallas as pl
from jax.experimental.pallas import tpu as pltpu
from jax.sharding import PartitionSpec as P

LOW = 256
PROJECT = 512
BASE = 32
CHUNK = 16
MESH = pl.DeviceIdType.MESH
F32 = jnp.float32
BF16 = jnp.bfloat16


def dense(values, weight):
    return jnp.maximum(jnp.dot(values, weight, preferred_element_type=F32), 0.0).astype(BF16)


def kernel(
    dims,
    x_hbm,
    bf_hbm,
    bs_hbm,
    bt_hbm,
    wt_hbm,
    nt_hbm,
    wi_hbm,
    wl_hbm,
    ni_hbm,
    nl_hbm,
    wp_hbm,
    np_hbm,
    tf_hbm,
    hid_ref,
    x_ref,
    bf_ref,
    wi_ref,
    wl_ref,
    ni_ref,
    nl_ref,
    bs,
    bt,
    wt,
    nt,
    wp,
    npj,
    tf,
    send_ids,
    recv_ids,
    counts,
    flat_wide,
    flat_narrow,
    give,
    got,
    part,
    recv_part,
    feats,
    local_sem,
    id_send,
    id_recv,
    part_send,
    part_recv,
    pair_send,
    pair_recv,
):
    n_table, n_row, span, tables, batch, slots, emb, rows = dims
    n = n_table * n_row
    lanes = batch * slots
    n_chunk = n // CHUNK
    owners = span * n_row
    my_table, my_row = lax.axis_index("table"), lax.axis_index("row")
    me = my_table * n_row + my_row
    own = my_table // span
    first_row = (lax.rem(my_table, span) * n_row + my_row) * rows

    def place(dev):
        return (dev // n_row, lax.rem(dev, n_row))

    def far_first(k, at, count):
        base = jnp.where(at < count // 2, count - 2 - k, k)
        return base + (base >= at).astype(jnp.int32)

    barrier = pltpu.get_barrier_semaphore()

    def greet(k, _):
        pl.semaphore_signal(
            barrier, inc=1, device_id=place(far_first(k, me, n)), device_id_type=MESH
        )
        return 0

    lax.fori_loop(0, n - 1, greet, 0, unroll=4)

    loads = [
        pltpu.make_async_copy(src, dst, local_sem.at[pos])
        for pos, (src, dst) in enumerate(
            [
                (wi_hbm, wi_ref),
                (wl_hbm, wl_ref),
                (ni_hbm, ni_ref),
                (nl_hbm, nl_ref),
                (x_hbm, x_ref),
                (bf_hbm, bf_ref),
                (bs_hbm, bs),
                (bt_hbm, bt),
                (tf_hbm, tf),
                (wp_hbm.at[own], wp),
                (np_hbm.at[own], npj),
                (wt_hbm, wt),
                (nt_hbm, nt),
            ]
        )
    ]
    for load in loads:
        load.start()

    for load in loads[:4]:
        load.wait()
    past = span * n_row * rows // LOW
    slot_at = lax.broadcasted_iota(jnp.int32, (slots, batch), 0)
    spread = (
        lax.rem(lax.broadcasted_iota(jnp.int32, (batch, lanes), 1), batch)
        == lax.broadcasted_iota(jnp.int32, (batch, lanes), 0)
    ).astype(F32).astype(BF16)
    diagonal = (
        lax.broadcasted_iota(jnp.int32, (slots, lanes), 1) // batch
        == lax.broadcasted_iota(jnp.int32, (slots, lanes), 0)
    )
    for t in range(tables):
        for kind, (i_ref, l_ref) in enumerate([(wi_ref, wl_ref), (ni_ref, nl_ref)]):
            ids = i_ref[t]
            high = jnp.where(slot_at < l_ref[t : t + 1, :], ids >> (LOW.bit_length() - 1), past)
            low = ids & (LOW - 1)
            high = jnp.dot(high.astype(F32).astype(BF16), spread, preferred_element_type=F32)
            low = jnp.dot(low.astype(F32).astype(BF16), spread, preferred_element_type=F32)
            row = jnp.sum(jnp.where(diagonal, high * LOW + low, 0.0), axis=0, keepdims=True)
            send_ids[t, kind : kind + 1, :] = row.astype(jnp.int32)

    pl.semaphore_wait(barrier, n - 1)

    def send_one(k, _):
        peer = far_first(k, me, n)
        pltpu.make_async_remote_copy(
            src_ref=send_ids.at[peer // n_row // span],
            dst_ref=recv_ids.at[me],
            send_sem=id_send,
            recv_sem=id_recv,
            device_id=place(peer),
            device_id_type=MESH,
        ).start()
        return 0

    lax.fori_loop(0, n - 1, send_one, 0, unroll=4)
    pltpu.make_async_copy(send_ids.at[own], recv_ids.at[me], id_recv).start()

    for load in loads[4:6]:
        load.wait()
    bottom = dense(x_ref[...], bf_ref[...])
    loads[6].wait()
    bottom = dense(bottom, bs[...])
    loads[7].wait()
    bottom = dense(bottom, bt[...])
    feats[0] = bottom.astype(F32)
    loads[8].wait()
    base = jnp.dot(bottom, tf[0:emb, :], preferred_element_type=F32)
    for load in loads[9:]:
        load.wait()

    high_count = rows // LOW
    high_rows = high_count * batch
    assert high_rows <= 256
    for r in range(0, rows, PROJECT):
        at = pl.ds(r, PROJECT)
        flat_wide[at, :] = jnp.dot(
            wt[at, :], wp[...], preferred_element_type=F32
        ).astype(BF16)
        flat_narrow[at, :] = lax.dot_general(
            nt[:, at], npj[...], (((0,), (0,)), ((), ())), preferred_element_type=F32
        ).astype(BF16)

    at_high = lax.broadcasted_iota(jnp.int32, (high_rows, lanes), 0).astype(F32).astype(BF16)
    at_low = lax.broadcasted_iota(jnp.int32, (LOW, lanes), 0).astype(F32).astype(BF16)
    one, zero = jnp.ones((), BF16), jnp.zeros((), BF16)
    marks = [one, jnp.full((), -BASE, BF16)]
    shift = jnp.full((), 192 * BASE, BF16)
    sample = lax.rem(lax.broadcasted_iota(jnp.int32, (1, lanes), 1), batch)

    pltpu.make_async_copy(recv_ids, recv_ids, id_recv).wait()

    def pooled(c):
        for k in range(CHUNK):
            ids = recv_ids[k * n_chunk + c] - first_row
            high, low = [], []
            for kind in range(2):
                local = ids[kind : kind + 1, :]
                key = (local >> (LOW.bit_length() - 1)) * batch + sample
                key = jnp.where((key >= 0) & (key < high_rows), key, -1)
                key = key.astype(F32).astype(BF16)
                digit = (local & (LOW - 1)).astype(F32).astype(BF16)
                high.append(jnp.where(key == at_high, marks[kind], zero))
                low.append(jnp.where(digit == at_low, one, zero))
            found = lax.dot_general(
                jnp.concatenate(high, axis=1),
                jnp.concatenate(low, axis=1),
                (((1,), (1,)), ((), ())),
                preferred_element_type=F32,
            ).astype(BF16)
            for h in range(high_count):
                counts[h, k * batch : (k + 1) * batch, :] = found[h * batch : (h + 1) * batch]
        wide = jnp.zeros((CHUNK * batch, emb), F32)
        narrow = jnp.zeros((CHUNK * batch, emb), F32)
        for h in range(high_count):
            both = counts[h]
            second = (both + shift) - shift
            first = both - second
            at = slice(h * LOW, (h + 1) * LOW)
            wide = wide + jnp.dot(first, flat_wide[at, :], preferred_element_type=F32)
            narrow = narrow + jnp.dot(second, flat_narrow[at, :], preferred_element_type=F32)
        narrow = narrow * (-1.0 / BASE)
        return wide.reshape(CHUNK, batch, emb), narrow.reshape(CHUNK, batch, emb)

    def pair_copy(c):
        return pltpu.make_async_remote_copy(
            src_ref=give.at[c],
            dst_ref=got.at[c],
            send_sem=pair_send.at[c],
            recv_sem=pair_recv.at[c],
            device_id=(my_table, 1 - my_row),
            device_id_type=MESH,
        )

    @pl.loop(0, n_chunk // n_row)
    def _(c):
        wide, narrow = pooled(c * n_row + 1 - my_row)
        give[c, :, :, 0:emb] = wide.astype(BF16)
        give[c, :, :, emb : 2 * emb] = narrow.astype(BF16)
        pair_copy(c).start()

    my_k = me // n_chunk

    @pl.loop(0, n_chunk // n_row)
    def _(c):
        wide, narrow = pooled(c * n_row + my_row)
        pair_copy(c).wait()
        part[c, :, :, 0:emb] = (wide + got[c, :, :, 0:emb].astype(F32)).astype(BF16)
        part[c, :, :, emb : 2 * emb] = (narrow + got[c, :, :, emb : 2 * emb].astype(F32)).astype(BF16)

        @pl.loop(0, CHUNK)
        def _(k):
            far = jnp.where(my_k < CHUNK // 2, CHUNK // 4 - 1 - k // 4, k // 4)
            k = far * 4 + lax.rem(my_k + k, 4)
            peer = k * n_chunk + c * n_row + my_row

            @pl.when(peer != me)
            def _():
                pltpu.make_async_remote_copy(
                    src_ref=part.at[c, k],
                    dst_ref=recv_part.at[my_table],
                    send_sem=part_send,
                    recv_sem=part_recv,
                    device_id=place(peer),
                    device_id_type=MESH,
                ).start()

            @pl.when(peer == me)
            def _():
                pltpu.make_async_copy(part.at[c, k], recv_part.at[my_table], part_recv).start()

    pltpu.make_async_copy(recv_part, recv_part, part_recv).wait()

    for t in range(tables):
        total = recv_part[t * span].astype(F32)
        for s in range(1, span):
            total = total + recv_part[t * span + s].astype(F32)
        total = total.astype(BF16).astype(F32)
        feats[1 + t] = total[:, 0:emb]
        feats[1 + tables + t] = total[:, emb : 2 * emb]

    features = 1 + 2 * tables
    pairs = features * (features - 1) // 2
    column = lax.broadcasted_iota(jnp.int32, (batch, pairs), 1)
    values = jnp.zeros((batch, pairs), F32)
    if features <= 16:
        held = [feats[f] for f in range(features)]
        pos = 0
        for f in range(features):
            for g in range(f + 1, features):
                value = jnp.sum(held[f] * held[g], axis=1, keepdims=True)
                values = jnp.where(column == pos, value, values)
                pos += 1
    else:

        def outer(f, values):
            mine = feats[f]
            start = f * features - f * (f + 1) // 2 - f - 1

            def inner(g, values):
                value = jnp.sum(mine * feats[g], axis=1, keepdims=True)
                return jnp.where(column == start + g, value, values)

            return lax.fori_loop(f + 1, features, inner, values)

        values = lax.fori_loop(0, features - 1, outer, values)
    hidden = base + jnp.dot(
        values.astype(BF16), tf[emb : emb + pairs, :], preferred_element_type=F32
    )
    hidden = jnp.maximum(hidden, 0.0).astype(BF16)
    hid_ref[...] = hidden

    pltpu.make_async_copy(
        recv_ids.at[pl.ds(0, n - 1)], recv_ids.at[pl.ds(0, n - 1)], id_send
    ).wait()
    pltpu.make_async_copy(
        recv_part.at[pl.ds(0, n_table - 1)], recv_part.at[pl.ds(0, n_table - 1)], part_send
    ).wait()


def last_kernel(hid_ref, tl_ref, out_ref, log_ref):
    out_ref[...] = hid_ref[...]
    total = jnp.zeros(log_ref.shape, F32)
    size = tl_ref.shape[1]
    for j in range(tl_ref.shape[0]):
        total = total + lax.dot_general(
            tl_ref[j : j + 1, :],
            hid_ref[:, j * size : (j + 1) * size],
            (((1,), (1,)), ((), ())),
            preferred_element_type=F32,
        )
    log_ref[...] = total


def body(
    dense_input,
    bottom_first,
    bottom_second,
    bottom_third,
    wide_tables,
    narrow_tables,
    wide_indices,
    wide_lengths,
    narrow_indices,
    narrow_lengths,
    wide_projection,
    narrow_projection,
    top_first,
    top_last,
):
    n_table, n_row = lax.axis_size("table"), lax.axis_size("row")
    tables = wide_projection.shape[0]
    span = n_table // tables
    n = n_table * n_row
    batch, slots = dense_input.shape[0], wide_indices.shape[2]
    emb = wide_projection.shape[2]
    rows, width = wide_tables.shape
    top = top_first.shape[1]
    dims = (n_table, n_row, span, tables, batch, slots, emb, rows)
    n_chunk = n // CHUNK
    vmem = pl.BlockSpec(memory_space=pltpu.VMEM)
    hbm = pl.BlockSpec(memory_space=pl.ANY)

    def like(a):
        return pltpu.VMEM(a.shape, a.dtype)

    hidden = pl.pallas_call(
        functools.partial(kernel, dims),
        out_shape=pltpu.VMEM((batch, top), BF16),
        in_specs=[hbm] * 13,
        out_specs=vmem,
        scratch_shapes=[
            like(dense_input),
            like(bottom_first),
            pltpu.VMEM((tables, slots, batch), jnp.int32),
            pltpu.VMEM((tables, batch), jnp.int32),
            pltpu.VMEM((tables, slots, batch), jnp.int32),
            pltpu.VMEM((tables, batch), jnp.int32),
            like(bottom_second),
            like(bottom_third),
            like(wide_tables),
            pltpu.VMEM(narrow_tables.shape[::-1], BF16),
            pltpu.VMEM(wide_projection.shape[1:], BF16),
            pltpu.VMEM(narrow_projection.shape[1:], BF16),
            like(top_first),
            pltpu.VMEM((tables, 2, batch * slots), jnp.int32),
            pltpu.VMEM((n, 2, batch * slots), jnp.int32),
            pltpu.VMEM((rows // LOW, CHUNK * batch, LOW), BF16),
            pltpu.VMEM((rows, emb), BF16),
            pltpu.VMEM((rows, emb), BF16),
            pltpu.VMEM((n_chunk // n_row, CHUNK, batch, 2 * emb), BF16),
            pltpu.VMEM((n_chunk // n_row, CHUNK, batch, 2 * emb), BF16),
            pltpu.VMEM((n_chunk // n_row, CHUNK, batch, 2 * emb), BF16),
            pltpu.VMEM((n_table, batch, 2 * emb), BF16),
            pltpu.VMEM((1 + 2 * tables, batch, emb), F32),
            pltpu.SemaphoreType.DMA((13,)),
            pltpu.SemaphoreType.DMA,
            pltpu.SemaphoreType.DMA,
            pltpu.SemaphoreType.DMA,
            pltpu.SemaphoreType.DMA,
            pltpu.SemaphoreType.DMA((n_chunk // n_row,)),
            pltpu.SemaphoreType.DMA((n_chunk // n_row,)),
        ],
        compiler_params=pltpu.CompilerParams(
            collective_id=0, has_side_effects=True, vmem_limit_bytes=int(60 * 2**20)
        ),
    )(
        dense_input,
        bottom_first,
        bottom_second,
        bottom_third,
        wide_tables,
        narrow_tables.T,
        wide_indices.transpose(1, 2, 0),
        wide_lengths.T,
        narrow_indices.transpose(1, 2, 0),
        narrow_lengths.T,
        wide_projection,
        narrow_projection,
        top_first,
    )
    hidden, logits = pl.pallas_call(
        last_kernel,
        out_shape=(
            jax.ShapeDtypeStruct((batch, top), BF16),
            jax.ShapeDtypeStruct((1, batch), F32),
        ),
        in_specs=[vmem, vmem],
        out_specs=(vmem, vmem),
        compiler_params=pltpu.CompilerParams(vmem_limit_bytes=4 * 2**20),
    )(hidden, top_last.reshape(-1, emb))
    return hidden, logits.reshape(-1)


def solution(mesh):
    split = ("table", "row")
    in_specs = (
        P(split, None),
        P(),
        P(),
        P(),
        P(split, None),
        P(split, None),
        P(split, None, None),
        P(split, None),
        P(split, None, None),
        P(split, None),
        P(),
        P(),
        P(),
        P(),
    )
    out_specs = (P(split, None), P(split))
    return jax.shard_map(body, mesh=mesh, in_specs=in_specs, out_specs=out_specs, check_vma=False)
```

```python
import functools

import jax
import jax.numpy as jnp
from jax import lax
from jax.experimental import pallas as pl
from jax.experimental.pallas import tpu as pltpu
from jax.sharding import PartitionSpec as P

LOW = 256
PROJECT = 512
BASE = 32
SIDES = 4
SIDE = 4
CHUNK = SIDES * SIDE
PLAN = ((0,0,None,None),(1,1,0,None),(2,2,1,0),(3,3,None,None),(None,None,3,1),(None,None,2,3),(None,None,None,2))
MESH = pl.DeviceIdType.MESH
F32 = jnp.float32
BF16 = jnp.bfloat16


def dense(values, weight):
    return jnp.maximum(jnp.dot(values, weight, preferred_element_type=F32), 0.0).astype(BF16)


def kernel(
    dims,
    x_hbm,
    bf_hbm,
    bs_hbm,
    bt_hbm,
    wt_hbm,
    nt_hbm,
    wi_hbm,
    wl_hbm,
    ni_hbm,
    nl_hbm,
    wp_hbm,
    np_hbm,
    tf_hbm,
    hid_ref,
    x_ref,
    bf_ref,
    wi_ref,
    wl_ref,
    ni_ref,
    nl_ref,
    bs,
    bt,
    wt,
    nt,
    wp,
    npj,
    tf,
    send_ids,
    recv_ids,
    counts,
    flat_wide,
    flat_narrow,
    give,
    got,
    keep,
    part,
    recv_part,
    feats,
    local_sem,
    id_send,
    id_recv,
    part_send,
    part_recv,
    pair_send,
    pair_recv,
):
    n_table, n_row, span, tables, batch, slots, emb, rows = dims
    n = n_table * n_row
    lanes = batch * slots
    n_chunk = n // CHUNK
    n_cc = n_chunk // n_row
    n_side = n_table // SIDES
    owners = span * n_row
    my_table, my_row = lax.axis_index("table"), lax.axis_index("row")
    me = my_table * n_row + my_row
    own = my_table // span
    first_row = (lax.rem(my_table, span) * n_row + my_row) * rows

    def place(dev):
        return (dev // n_row, lax.rem(dev, n_row))

    def far_first(k, at, count):
        base = jnp.where(at < count // 2, count - 2 - k, k)
        return base + (base >= at).astype(jnp.int32)

    barrier = pltpu.get_barrier_semaphore()

    def greet(k, _):
        pl.semaphore_signal(
            barrier, inc=1, device_id=place(far_first(k, me, n)), device_id_type=MESH
        )
        return 0

    lax.fori_loop(0, n - 1, greet, 0, unroll=4)

    loads = [
        pltpu.make_async_copy(src, dst, local_sem.at[pos])
        for pos, (src, dst) in enumerate(
            [
                (wi_hbm, wi_ref),
                (wl_hbm, wl_ref),
                (ni_hbm, ni_ref),
                (nl_hbm, nl_ref),
                (x_hbm, x_ref),
                (bf_hbm, bf_ref),
                (bs_hbm, bs),
                (bt_hbm, bt),
                (tf_hbm, tf),
                (wp_hbm.at[own], wp),
                (np_hbm.at[own], npj),
                (wt_hbm, wt),
                (nt_hbm, nt),
            ]
        )
    ]
    for load in loads:
        load.start()

    for load in loads[:4]:
        load.wait()
    past = span * n_row * rows // LOW
    slot_at = lax.broadcasted_iota(jnp.int32, (slots, batch), 0)
    spread = (
        lax.rem(lax.broadcasted_iota(jnp.int32, (batch, lanes), 1), batch)
        == lax.broadcasted_iota(jnp.int32, (batch, lanes), 0)
    ).astype(F32).astype(BF16)
    diagonal = (
        lax.broadcasted_iota(jnp.int32, (slots, lanes), 1) // batch
        == lax.broadcasted_iota(jnp.int32, (slots, lanes), 0)
    )
    for t in range(tables):
        for kind, (i_ref, l_ref) in enumerate([(wi_ref, wl_ref), (ni_ref, nl_ref)]):
            ids = i_ref[t]
            high = jnp.where(slot_at < l_ref[t : t + 1, :], ids >> (LOW.bit_length() - 1), past)
            low = ids & (LOW - 1)
            high = jnp.dot(high.astype(F32).astype(BF16), spread, preferred_element_type=F32)
            low = jnp.dot(low.astype(F32).astype(BF16), spread, preferred_element_type=F32)
            row = jnp.sum(jnp.where(diagonal, high * LOW + low, 0.0), axis=0, keepdims=True)
            send_ids[t, kind : kind + 1, :] = row.astype(jnp.int32)

    pl.semaphore_wait(barrier, n - 1)

    def send_one(k, _):
        peer = me ^ jnp.where(k < n // 2, n // 2 + k, k + 1 - n // 2)
        pltpu.make_async_remote_copy(
            src_ref=send_ids.at[peer // n_row // span],
            dst_ref=recv_ids.at[me],
            send_sem=id_send,
            recv_sem=id_recv.at[my_table // n_side],
            device_id=place(peer),
            device_id_type=MESH,
        ).start()
        return 0

    lax.fori_loop(0, n - 1, send_one, 0, unroll=4)
    pltpu.make_async_copy(send_ids.at[own], recv_ids.at[me], id_recv.at[my_table // n_side]).start()

    for load in loads[4:6]:
        load.wait()
    bottom = dense(x_ref[...], bf_ref[...])
    loads[6].wait()
    bottom = dense(bottom, bs[...])
    loads[7].wait()
    bottom = dense(bottom, bt[...])
    feats[0] = bottom.astype(F32)
    loads[8].wait()
    base = jnp.dot(bottom, tf[0:emb, :], preferred_element_type=F32)
    for load in loads[9:]:
        load.wait()

    high_count = rows // LOW
    high_rows = high_count * batch
    assert high_rows <= 256
    for r in range(0, rows, PROJECT):
        at = pl.ds(r, PROJECT)
        flat_wide[at, :] = jnp.dot(
            wt[at, :], wp[...], preferred_element_type=F32
        ).astype(BF16)
        narrow = lax.dot_general(
            nt[:, at], npj[...], (((0,), (0,)), ((), ())), preferred_element_type=F32
        )
        flat_narrow[at, :] = (narrow * (-1.0 / BASE)).astype(BF16)

    at_high = lax.broadcasted_iota(jnp.int32, (high_rows, lanes), 0).astype(F32).astype(BF16)
    at_low = lax.broadcasted_iota(jnp.int32, (LOW, lanes), 0).astype(F32).astype(BF16)
    one, zero = jnp.ones((), BF16), jnp.zeros((), BF16)
    marks = [one, jnp.full((), -BASE, BF16)]
    shift = jnp.full((), 192 * BASE, BF16)
    sample = lax.rem(lax.broadcasted_iota(jnp.int32, (1, lanes), 1), batch)

    my_side = my_table // n_side

    def side_of(step):
        if not step:
            return my_side
        side = SIDES - step
        return jnp.where(side > my_side, side, side - 1)

    def each(body):
        if n_cc == 1:
            body(0)
        else:
            pl.loop(0, n_cc)(body)

    def count(step, cc):
        first_k = side_of(step) * SIDE
        for place_row in range(n_row):
            row = lax.rem(my_row + place_row, n_row)
            for k in range(SIDE):
                at = (place_row * SIDE + k) * batch
                ids = recv_ids[(first_k + k) * n_chunk + cc * n_row + row] - first_row
                high, low = [], []
                for kind in range(2):
                    local = ids[kind : kind + 1, :]
                    key = (local >> (LOW.bit_length() - 1)) * batch + sample
                    key = jnp.where((key >= 0) & (key < high_rows), key, -1)
                    key = key.astype(F32).astype(BF16)
                    digit = (local & (LOW - 1)).astype(F32).astype(BF16)
                    high.append(jnp.where(key == at_high, marks[kind], zero))
                    low.append(jnp.where(digit == at_low, one, zero))
                found = lax.dot_general(
                    jnp.concatenate(high, axis=1),
                    jnp.concatenate(low, axis=1),
                    (((1,), (1,)), ((), ())),
                    preferred_element_type=F32,
                ).astype(BF16)
                for h in range(high_count):
                    counts[step, cc, h, at : at + batch, :] = found[h * batch : (h + 1) * batch]

    def weigh(step, cc):
        wide = jnp.zeros((SIDE * n_row * batch, emb), F32)
        narrow = jnp.zeros((SIDE * n_row * batch, emb), F32)
        for h in range(high_count):
            both = counts[step, cc, h]
            second = (both + shift) - shift
            first = both - second
            at = slice(h * LOW, (h + 1) * LOW)
            wide = wide + jnp.dot(first, flat_wide[at, :], preferred_element_type=F32)
            narrow = narrow + jnp.dot(second, flat_narrow[at, :], preferred_element_type=F32)
        given = SIDE * batch
        for half, value in enumerate((wide, narrow)):
            at = slice(half * emb, (half + 1) * emb)
            give[step, cc, :, at] = value[:given].astype(BF16)
            keep[step, cc, :, at] = value[given:]
        pair_copy(step, cc).start()

    def pair_copy(step, cc):
        return pltpu.make_async_remote_copy(
            src_ref=give.at[step, cc],
            dst_ref=got.at[step, cc],
            send_sem=pair_send.at[step, cc],
            recv_sem=pair_recv.at[step, cc],
            device_id=(my_table, 1 - my_row),
            device_id_type=MESH,
        )

    def arrive(step):
        side = side_of(step)
        arrived = recv_ids.at[pl.ds(side * (n // SIDES), n // SIDES)]
        pltpu.make_async_copy(arrived, arrived, id_recv.at[side]).wait()

    def finish(step):
        side = side_of(step)

        def block(cc):
            pair_copy(step, cc).wait()
            part[step, cc] = (keep[step, cc] + got[step, cc].astype(F32)).astype(BF16)
            for k in range(SIDE):
                peer = (side * SIDE + k) * n_cc + cc

                pltpu.make_async_remote_copy(
                    src_ref=part.at[step, cc, pl.ds(k * batch, batch)],
                    dst_ref=recv_part.at[my_table],
                    send_sem=part_send,
                    recv_sem=part_recv,
                    device_id=(peer, 1 - my_row),
                    device_id_type=MESH,
                ).start()

        each(block)

    for waits, counted, weighed, finished in PLAN:
        if waits is not None:
            arrive(waits)

        def block(cc):
            if counted is not None:
                count(counted, cc)
            if weighed is not None:
                weigh(weighed, cc)

        each(block)
        if finished is not None:
            finish(finished)

    pltpu.make_async_copy(recv_part, recv_part, part_recv).wait()

    for t in range(tables):
        total = recv_part[t * span].astype(F32)
        for s in range(1, span):
            total = total + recv_part[t * span + s].astype(F32)
        total = total.astype(BF16).astype(F32)
        feats[1 + t] = total[:, 0:emb]
        feats[1 + tables + t] = total[:, emb : 2 * emb]

    features = 1 + 2 * tables
    pairs = features * (features - 1) // 2
    column = lax.broadcasted_iota(jnp.int32, (batch, pairs), 1)
    values = jnp.zeros((batch, pairs), F32)
    if features <= 16:
        held = [feats[f] for f in range(features)]
        pos = 0
        for f in range(features):
            for g in range(f + 1, features):
                value = jnp.sum(held[f] * held[g], axis=1, keepdims=True)
                values = jnp.where(column == pos, value, values)
                pos += 1
    else:

        def outer(f, values):
            mine = feats[f]
            start = f * features - f * (f + 1) // 2 - f - 1

            def inner(g, values):
                value = jnp.sum(mine * feats[g], axis=1, keepdims=True)
                return jnp.where(column == start + g, value, values)

            return lax.fori_loop(f + 1, features, inner, values)

        values = lax.fori_loop(0, features - 1, outer, values)
    hidden = base + jnp.dot(
        values.astype(BF16), tf[emb : emb + pairs, :], preferred_element_type=F32
    )
    hidden = jnp.maximum(hidden, 0.0).astype(BF16)
    hid_ref[...] = hidden

    pltpu.make_async_copy(
        recv_ids.at[pl.ds(0, n - 1)], recv_ids.at[pl.ds(0, n - 1)], id_send
    ).wait()
    pltpu.make_async_copy(recv_part, recv_part, part_send).wait()


def last_kernel(hid_ref, tl_ref, out_ref, log_ref):
    out_ref[...] = hid_ref[...]
    total = jnp.zeros(log_ref.shape, F32)
    size = tl_ref.shape[1]
    for j in range(tl_ref.shape[0]):
        total = total + lax.dot_general(
            tl_ref[j : j + 1, :],
            hid_ref[:, j * size : (j + 1) * size],
            (((1,), (1,)), ((), ())),
            preferred_element_type=F32,
        )
    log_ref[...] = total


def body(
    dense_input,
    bottom_first,
    bottom_second,
    bottom_third,
    wide_tables,
    narrow_tables,
    wide_indices,
    wide_lengths,
    narrow_indices,
    narrow_lengths,
    wide_projection,
    narrow_projection,
    top_first,
    top_last,
):
    n_table, n_row = lax.axis_size("table"), lax.axis_size("row")
    tables = wide_projection.shape[0]
    span = n_table // tables
    n = n_table * n_row
    batch, slots = dense_input.shape[0], wide_indices.shape[2]
    emb = wide_projection.shape[2]
    rows, width = wide_tables.shape
    top = top_first.shape[1]
    dims = (n_table, n_row, span, tables, batch, slots, emb, rows)
    n_cc = n // CHUNK // n_row
    vmem = pl.BlockSpec(memory_space=pltpu.VMEM)
    hbm = pl.BlockSpec(memory_space=pl.ANY)

    def like(a):
        return pltpu.VMEM(a.shape, a.dtype)

    hidden = pl.pallas_call(
        functools.partial(kernel, dims),
        out_shape=pltpu.VMEM((batch, top), BF16),
        in_specs=[hbm] * 13,
        out_specs=vmem,
        scratch_shapes=[
            like(dense_input),
            like(bottom_first),
            pltpu.VMEM((tables, slots, batch), jnp.int32),
            pltpu.VMEM((tables, batch), jnp.int32),
            pltpu.VMEM((tables, slots, batch), jnp.int32),
            pltpu.VMEM((tables, batch), jnp.int32),
            like(bottom_second),
            like(bottom_third),
            like(wide_tables),
            pltpu.VMEM(narrow_tables.shape[::-1], BF16),
            pltpu.VMEM(wide_projection.shape[1:], BF16),
            pltpu.VMEM(narrow_projection.shape[1:], BF16),
            like(top_first),
            pltpu.VMEM((tables, 2, batch * slots), jnp.int32),
            pltpu.VMEM((n, 2, batch * slots), jnp.int32),
            pltpu.VMEM((SIDES, n_cc, rows // LOW, SIDE * n_row * batch, LOW), BF16),
            pltpu.VMEM((rows, emb), BF16),
            pltpu.VMEM((rows, emb), BF16),
            *[pltpu.VMEM((SIDES, n_cc, SIDE * batch, 2 * emb), d) for d in (BF16, BF16, F32, BF16)],
            pltpu.VMEM((n_table, batch, 2 * emb), BF16),
            pltpu.VMEM((1 + 2 * tables, batch, emb), F32),
            pltpu.SemaphoreType.DMA((13,)),
            pltpu.SemaphoreType.DMA,
            pltpu.SemaphoreType.DMA((SIDES,)),
            pltpu.SemaphoreType.DMA,
            pltpu.SemaphoreType.DMA,
            pltpu.SemaphoreType.DMA((SIDES, n_cc)),
            pltpu.SemaphoreType.DMA((SIDES, n_cc)),
        ],
        compiler_params=pltpu.CompilerParams(
            collective_id=0, has_side_effects=True, vmem_limit_bytes=int(60 * 2**20)
        ),
    )(
        dense_input,
        bottom_first,
        bottom_second,
        bottom_third,
        wide_tables,
        narrow_tables.T,
        wide_indices.transpose(1, 2, 0),
        wide_lengths.T,
        narrow_indices.transpose(1, 2, 0),
        narrow_lengths.T,
        wide_projection,
        narrow_projection,
        top_first,
    )
    hidden, logits = pl.pallas_call(
        last_kernel,
        out_shape=(
            jax.ShapeDtypeStruct((batch, top), BF16),
            jax.ShapeDtypeStruct((1, batch), F32),
        ),
        in_specs=[vmem, vmem],
        out_specs=(vmem, vmem),
        compiler_params=pltpu.CompilerParams(vmem_limit_bytes=4 * 2**20),
    )(hidden, top_last.reshape(-1, emb))
    return hidden, logits.reshape(-1)


def solution(mesh):
    split = ("table", "row")
    in_specs = (
        P(split, None),
        P(),
        P(),
        P(),
        P(split, None),
        P(split, None),
        P(split, None, None),
        P(split, None),
        P(split, None, None),
        P(split, None),
        P(),
        P(),
        P(),
        P(),
    )
    out_specs = (P(split, None), P(split))
    return jax.shard_map(body, mesh=mesh, in_specs=in_specs, out_specs=out_specs, check_vma=False)
```

```python
import functools

import jax
import jax.numpy as jnp
from jax import lax
from jax.experimental import pallas as pl
from jax.experimental.pallas import tpu as pltpu
from jax.sharding import PartitionSpec as P

LOW = 256
PROJECT = 512
BASE = 32
SIDES = 4
SIDE = 4
CHUNK = SIDES * SIDE
PLAN = ((((0, 0), (0, 1)), ((0, 0), (0, 1)), None, None),(((1, 0), (1, 1)), ((1, 0), (1, 1)), None, None),(((2, 0), (2, 1)), ((2, 0), (2, 1)), None, None),(((3, 1),), ((3, 1),), None, None),(((3, 0),), ((3, 0),), None, None),((), (), 1, None),((), (), 0, 1),((), (), None, 0))
MESH = pl.DeviceIdType.MESH
F32 = jnp.float32
BF16 = jnp.bfloat16
F8 = jnp.float8_e4m3fn


def dense(values, weight):
    return jnp.maximum(jnp.dot(values, weight, preferred_element_type=F32), 0.0).astype(BF16)


def kernel(
    dims,
    x_hbm,
    bf_hbm,
    bs_hbm,
    bt_hbm,
    wt_hbm,
    nt_hbm,
    wi_hbm,
    wl_hbm,
    ni_hbm,
    nl_hbm,
    wp_hbm,
    np_hbm,
    tf_hbm,
    hid_ref,
    x_ref,
    bf_ref,
    wi_ref,
    wl_ref,
    ni_ref,
    nl_ref,
    bs,
    bt,
    wt,
    nt,
    wp,
    npj,
    tf,
    send_ids,
    recv_ids,
    counts,
    flat_wide,
    flat_narrow,
    give,
    got,
    keep,
    part,
    recv_part,
    feats,
    local_sem,
    id_send,
    id_recv,
    part_send,
    part_recv,
    pair_send,
    pair_recv,
):
    n_table, n_row, span, tables, batch, slots, emb, rows = dims
    n = n_table * n_row
    lanes = batch * slots
    n_chunk = n // CHUNK
    n_cc = n_chunk // n_row
    n_side = n_table // SIDES
    owners = span * n_row
    my_table, my_row = lax.axis_index("table"), lax.axis_index("row")
    me = my_table * n_row + my_row
    own = my_table // span
    first_row = (lax.rem(my_table, span) * n_row + my_row) * rows

    def place(dev):
        return (dev // n_row, lax.rem(dev, n_row))

    def far_first(k, at, count):
        base = jnp.where(at < count // 2, count - 2 - k, k)
        return base + (base >= at).astype(jnp.int32)

    barrier = pltpu.get_barrier_semaphore()

    def greet(k, _):
        pl.semaphore_signal(
            barrier, inc=1, device_id=place(far_first(k, me, n)), device_id_type=MESH
        )
        return 0

    lax.fori_loop(0, n - 1, greet, 0, unroll=4)

    loads = [
        pltpu.make_async_copy(src, dst, local_sem.at[pos])
        for pos, (src, dst) in enumerate(
            [
                (wi_hbm, wi_ref),
                (wl_hbm, wl_ref),
                (ni_hbm, ni_ref),
                (nl_hbm, nl_ref),
                (x_hbm, x_ref),
                (bf_hbm, bf_ref),
                (bs_hbm, bs),
                (bt_hbm, bt),
                (tf_hbm, tf),
                (wp_hbm.at[own], wp),
                (np_hbm.at[own], npj),
                (wt_hbm, wt),
                (nt_hbm, nt),
            ]
        )
    ]
    for load in loads:
        load.start()

    for load in loads[:4]:
        load.wait()
    past = span * n_row * rows // LOW
    slot_at = lax.broadcasted_iota(jnp.int32, (slots, batch), 0)
    spread = (
        lax.rem(lax.broadcasted_iota(jnp.int32, (batch, lanes), 1), batch)
        == lax.broadcasted_iota(jnp.int32, (batch, lanes), 0)
    ).astype(F32).astype(BF16)
    diagonal = (
        lax.broadcasted_iota(jnp.int32, (slots, lanes), 1) // batch
        == lax.broadcasted_iota(jnp.int32, (slots, lanes), 0)
    )
    for t in range(tables):
        for kind, (i_ref, l_ref) in enumerate([(wi_ref, wl_ref), (ni_ref, nl_ref)]):
            ids = i_ref[t]
            high = jnp.where(slot_at < l_ref[t : t + 1, :], ids >> (LOW.bit_length() - 1), past)
            low = ids & (LOW - 1)
            high = jnp.dot(high.astype(F32).astype(BF16), spread, preferred_element_type=F32)
            low = jnp.dot(low.astype(F32).astype(BF16), spread, preferred_element_type=F32)
            row = jnp.sum(jnp.where(diagonal, high * LOW + low, 0.0), axis=0, keepdims=True)
            send_ids[t, kind : kind + 1, :] = row.astype(jnp.int32)

    pl.semaphore_wait(barrier, n - 1)

    def send_one(k, _):
        peer = me ^ jnp.where(k < n // 2, n // 2 + k, k + 1 - n // 2)
        pltpu.make_async_remote_copy(
            src_ref=send_ids.at[peer // n_row // span],
            dst_ref=recv_ids.at[my_row, my_table],
            send_sem=id_send,
            recv_sem=id_recv.at[my_table // n_side, my_row],
            device_id=place(peer),
            device_id_type=MESH,
        ).start()
        return 0

    lax.fori_loop(0, n - 1, send_one, 0, unroll=4)
    pltpu.make_async_copy(
        send_ids.at[own], recv_ids.at[my_row, my_table], id_recv.at[my_table // n_side, my_row]
    ).start()

    for load in loads[4:6]:
        load.wait()
    bottom = dense(x_ref[...], bf_ref[...])
    loads[6].wait()
    bottom = dense(bottom, bs[...])
    loads[7].wait()
    bottom = dense(bottom, bt[...])
    feats[0] = bottom.astype(F32)
    loads[8].wait()
    base = jnp.dot(bottom, tf[0:emb, :], preferred_element_type=F32)
    for load in loads[9:]:
        load.wait()

    high_count = rows // LOW
    high_rows = high_count * batch
    assert high_rows <= 256
    for r in range(0, rows, PROJECT):
        at = pl.ds(r, PROJECT)
        flat_wide[:, at] = lax.dot_general(
            wp[...], wt[at, :], (((0,), (1,)), ((), ())), preferred_element_type=F32
        ).astype(BF16)
        narrow = lax.dot_general(
            npj[...], nt[:, at], (((0,), (0,)), ((), ())), preferred_element_type=F32
        )
        flat_narrow[:, at] = (narrow * (-1.0 / BASE)).astype(BF16)

    at_high = lax.broadcasted_iota(jnp.int32, (high_rows, lanes), 0).astype(F32).astype(BF16)
    at_low = lax.broadcasted_iota(jnp.int32, (LOW, lanes), 0).astype(F32).astype(BF16)
    one, zero = jnp.ones((), BF16), jnp.zeros((), BF16)
    marks = [one, jnp.full((), -BASE, BF16)]
    shift = jnp.full((), 192 * BASE, BF16)
    sample = lax.rem(lax.broadcasted_iota(jnp.int32, (1, lanes), 1), batch)

    my_side = my_table // n_side

    def side_of(step):
        if not step:
            return my_side
        side = SIDES - step
        return jnp.where(side > my_side, side, side - 1)

    def each(body):
        if n_cc == 1:
            body(0)
        else:
            pl.loop(0, n_cc)(body)

    def taken(row, table):
        ids = recv_ids[row, table] - first_row
        high, low = [], []
        for kind in range(2):
            local = ids[kind : kind + 1, :]
            key = (local >> (LOW.bit_length() - 1)) * batch + sample
            key = jnp.where((key >= 0) & (key < high_rows), key, -1)
            key = key.astype(F32).astype(BF16)
            digit = (local & (LOW - 1)).astype(F32).astype(BF16)
            high.append(jnp.where(key == at_high, marks[kind], zero))
            low.append(jnp.where(digit == at_low, one, zero))
        both = lax.dot_general(
            jnp.concatenate(high, axis=1),
            jnp.concatenate(low, axis=1),
            (((1,), (1,)), ((), ())),
            preferred_element_type=F32,
        ).astype(BF16)
        second = (both + shift) - shift
        return both - second, second

    def count(step, row, cc):
        first_k = side_of(step) * SIDE
        mine = jnp.where(row == my_row, 0, 1)
        for k in range(0, SIDE, 2):
            table = (first_k + k) * n_cc + cc
            at = pl.multiple_of(mine * 2 * SIDE * batch, 2 * SIDE * batch)
            at = pl.ds(at + ((step % 2) * SIDE + k) * batch, 2 * batch)
            found = zip(taken(row, table), taken(row, table + n_cc))
            for kind, (here, there) in enumerate(found):
                for h in range(high_count):
                    own_rows = slice(h * batch, (h + 1) * batch)
                    counts[step // 2, cc, kind, h, at, :] = jnp.concatenate(
                        [here[own_rows], there[own_rows]], axis=0
                    ).astype(F8)

    def weigh(turn, cc):
        given = 2 * SIDE * batch
        for kind, flat in enumerate((flat_wide, flat_narrow)):
            total = jnp.zeros((emb, n_row * given), F32)
            for h in range(high_count):
                total = total + lax.dot_general(
                    flat[:, h * LOW : (h + 1) * LOW],
                    counts[turn, cc, kind, h],
                    (((1,), (1,)), ((), ())),
                    preferred_element_type=F32,
                )
            total = total.T
            at = slice(kind * emb, (kind + 1) * emb)
            give[turn, cc, :, at] = total[:given].astype(BF16)
            keep[turn, cc, :, at] = total[given:]
        pair_copy(turn, cc).start()

    def pair_copy(step, cc):
        return pltpu.make_async_remote_copy(
            src_ref=give.at[step, cc],
            dst_ref=got.at[step, cc],
            send_sem=pair_send.at[step, cc],
            recv_sem=pair_recv.at[step, cc],
            device_id=(my_table, 1 - my_row),
            device_id_type=MESH,
        )

    def arrive(step, row):
        side = side_of(step)
        arrived = recv_ids.at[row, pl.ds(side * n_side, n_side)]
        pltpu.make_async_copy(arrived, arrived, id_recv.at[side, row]).wait()

    def finish(turn):
        def block(cc):
            pair_copy(turn, cc).wait()
            part[turn, cc] = (keep[turn, cc] + got[turn, cc].astype(F32)).astype(BF16)
            for half in (1, 0):
                side = side_of(2 * turn + half)
                for k in range(SIDE):
                    peer = (side * SIDE + k) * n_cc + cc
                    at = (half * SIDE + k) * batch
                    pltpu.make_async_remote_copy(
                        src_ref=part.at[turn, cc, pl.ds(at, batch)],
                        dst_ref=recv_part.at[my_table],
                        send_sem=part_send,
                        recv_sem=part_recv,
                        device_id=(peer, 1 - my_row),
                        device_id_type=MESH,
                    ).start()

        each(block)

    for waits, counted, weighed, finished in PLAN:
        for step, row in waits:
            arrive(step, row)

        def block(cc):
            for step, row in counted:
                count(step, row, cc)
            if weighed is not None:
                weigh(weighed, cc)

        each(block)
        if finished is not None:
            finish(finished)

    pltpu.make_async_copy(recv_part, recv_part, part_recv).wait()

    for t in range(tables):
        total = recv_part[t * span].astype(F32)
        for s in range(1, span):
            total = total + recv_part[t * span + s].astype(F32)
        total = total.astype(BF16).astype(F32)
        feats[1 + t] = total[:, 0:emb]
        feats[1 + tables + t] = total[:, emb : 2 * emb]

    features = 1 + 2 * tables
    pairs = features * (features - 1) // 2
    column = lax.broadcasted_iota(jnp.int32, (batch, pairs), 1)
    values = jnp.zeros((batch, pairs), F32)
    if features <= 16:
        held = [feats[f] for f in range(features)]
        pos = 0
        for f in range(features):
            for g in range(f + 1, features):
                value = jnp.sum(held[f] * held[g], axis=1, keepdims=True)
                values = jnp.where(column == pos, value, values)
                pos += 1
    else:

        def outer(f, values):
            mine = feats[f]
            start = f * features - f * (f + 1) // 2 - f - 1

            def inner(g, values):
                value = jnp.sum(mine * feats[g], axis=1, keepdims=True)
                return jnp.where(column == start + g, value, values)

            return lax.fori_loop(f + 1, features, inner, values)

        values = lax.fori_loop(0, features - 1, outer, values)
    hidden = base + jnp.dot(
        values.astype(BF16), tf[emb : emb + pairs, :], preferred_element_type=F32
    )
    hidden = jnp.maximum(hidden, 0.0).astype(BF16)
    hid_ref[...] = hidden

    for row in range(n_row):
        left = recv_ids.at[row, pl.ds(0, n_table - (1 if row else 0))]
        pltpu.make_async_copy(left, left, id_send).wait()
    pltpu.make_async_copy(recv_part, recv_part, part_send).wait()


def last_kernel(hid_ref, tl_ref, out_ref, log_ref):
    out_ref[...] = hid_ref[...]
    total = jnp.zeros(log_ref.shape, F32)
    size = tl_ref.shape[1]
    for j in range(tl_ref.shape[0]):
        total = total + lax.dot_general(
            tl_ref[j : j + 1, :],
            hid_ref[:, j * size : (j + 1) * size],
            (((1,), (1,)), ((), ())),
            preferred_element_type=F32,
        )
    log_ref[...] = total


def body(
    dense_input,
    bottom_first,
    bottom_second,
    bottom_third,
    wide_tables,
    narrow_tables,
    wide_indices,
    wide_lengths,
    narrow_indices,
    narrow_lengths,
    wide_projection,
    narrow_projection,
    top_first,
    top_last,
):
    n_table, n_row = lax.axis_size("table"), lax.axis_size("row")
    tables = wide_projection.shape[0]
    span = n_table // tables
    n = n_table * n_row
    batch, slots = dense_input.shape[0], wide_indices.shape[2]
    emb = wide_projection.shape[2]
    rows, width = wide_tables.shape
    top = top_first.shape[1]
    dims = (n_table, n_row, span, tables, batch, slots, emb, rows)
    n_cc = n // CHUNK // n_row
    vmem = pl.BlockSpec(memory_space=pltpu.VMEM)
    hbm = pl.BlockSpec(memory_space=pl.ANY)

    def like(a):
        return pltpu.VMEM(a.shape, a.dtype)

    hidden = pl.pallas_call(
        functools.partial(kernel, dims),
        out_shape=pltpu.VMEM((batch, top), BF16),
        in_specs=[hbm] * 13,
        out_specs=vmem,
        scratch_shapes=[
            like(dense_input),
            like(bottom_first),
            pltpu.VMEM((tables, slots, batch), jnp.int32),
            pltpu.VMEM((tables, batch), jnp.int32),
            pltpu.VMEM((tables, slots, batch), jnp.int32),
            pltpu.VMEM((tables, batch), jnp.int32),
            like(bottom_second),
            like(bottom_third),
            like(wide_tables),
            pltpu.VMEM(narrow_tables.shape[::-1], BF16),
            pltpu.VMEM(wide_projection.shape[1:], BF16),
            pltpu.VMEM(narrow_projection.shape[1:], BF16),
            like(top_first),
            pltpu.VMEM((tables, 2, batch * slots), jnp.int32),
            pltpu.VMEM((n_row, n_table, 2, batch * slots), jnp.int32),
            pltpu.VMEM((2, n_cc, 2, rows // LOW, 2 * SIDE * n_row * batch, LOW), F8),
            pltpu.VMEM((emb, rows), BF16),
            pltpu.VMEM((emb, rows), BF16),
            *[pltpu.VMEM((2, n_cc, 2 * SIDE * batch, 2 * emb), d) for d in (BF16, BF16, F32, BF16)],
            pltpu.VMEM((n_table, batch, 2 * emb), BF16),
            pltpu.VMEM((1 + 2 * tables, batch, emb), F32),
            pltpu.SemaphoreType.DMA((13,)),
            pltpu.SemaphoreType.DMA,
            pltpu.SemaphoreType.DMA((SIDES, n_row)),
            pltpu.SemaphoreType.DMA,
            pltpu.SemaphoreType.DMA,
            pltpu.SemaphoreType.DMA((2, n_cc)),
            pltpu.SemaphoreType.DMA((2, n_cc)),
        ],
        compiler_params=pltpu.CompilerParams(
            collective_id=0, has_side_effects=True, vmem_limit_bytes=int(60 * 2**20)
        ),
    )(
        dense_input,
        bottom_first,
        bottom_second,
        bottom_third,
        wide_tables,
        narrow_tables.T,
        wide_indices.transpose(1, 2, 0),
        wide_lengths.T,
        narrow_indices.transpose(1, 2, 0),
        narrow_lengths.T,
        wide_projection,
        narrow_projection,
        top_first,
    )
    hidden, logits = pl.pallas_call(
        last_kernel,
        out_shape=(
            jax.ShapeDtypeStruct((batch, top), BF16),
            jax.ShapeDtypeStruct((1, batch), F32),
        ),
        in_specs=[vmem, vmem],
        out_specs=(vmem, vmem),
        compiler_params=pltpu.CompilerParams(vmem_limit_bytes=4 * 2**20),
    )(hidden, top_last.reshape(-1, emb))
    return hidden, logits.reshape(-1)


def solution(mesh):
    split = ("table", "row")
    in_specs = (
        P(split, None),
        P(),
        P(),
        P(),
        P(split, None),
        P(split, None),
        P(split, None, None),
        P(split, None),
        P(split, None, None),
        P(split, None),
        P(),
        P(),
        P(),
        P(),
    )
    out_specs = (P(split, None), P(split))
    return jax.shard_map(body, mesh=mesh, in_specs=in_specs, out_specs=out_specs, check_vma=False)
```

```python
import functools

import jax
import jax.numpy as jnp
from jax import lax
from jax.experimental import pallas as pl
from jax.experimental.pallas import tpu as pltpu
from jax.sharding import PartitionSpec as P

LOW = 256
PROJECT = 1024
BASE = 32
SIDES = 4
SIDE = 4
CHUNK = SIDES * SIDE
PLAN = ((((0, 0), (0, 1)), ((0, 0), (0, 1)), (), ()), (((2, 0), (2, 1)), ((2, 0), (2, 1)), (), ()), (((3, 1),), ((3, 1),), (), ()), (((3, 0),), ((3, 0),), (), ()), ((), (), (1,), ()), (((1, 0), (1, 1)), ((1, 0), (1, 1)), (), ()), ((), (), (), (1,)), ((), (), (0,), ()), ((), (), (), (0,)))
MESH = pl.DeviceIdType.MESH
F32 = jnp.float32
BF16 = jnp.bfloat16
F8 = jnp.float8_e4m3fn


def dense(values, weight):
    return jnp.maximum(jnp.dot(values, weight, preferred_element_type=F32), 0.0).astype(BF16)


def kernel(
    dims,
    x_hbm,
    bf_hbm,
    bs_hbm,
    bt_hbm,
    wt_hbm,
    nt_hbm,
    wi_hbm,
    wl_hbm,
    ni_hbm,
    nl_hbm,
    wp_hbm,
    np_hbm,
    tf_hbm,
    hid_ref,
    x_ref,
    bf_ref,
    wi_ref,
    wl_ref,
    ni_ref,
    nl_ref,
    bs,
    bt,
    wt,
    nt,
    wp,
    npj,
    tf,
    send_ids,
    recv_ids,
    counts,
    flat_wide,
    flat_narrow,
    give,
    got,
    keep,
    part,
    recv_part,
    feats,
    local_sem,
    id_send,
    id_recv,
    part_send,
    part_recv,
    pair_send,
    pair_recv,
):
    n_table, n_row, span, tables, batch, slots, emb, rows = dims
    n = n_table * n_row
    lanes = batch * slots
    n_chunk = n // CHUNK
    n_cc = n_chunk // n_row
    n_side = n_table // SIDES
    owners = span * n_row
    my_table, my_row = lax.axis_index("table"), lax.axis_index("row")
    me = my_table * n_row + my_row
    own = my_table // span
    first_row = (lax.rem(my_table, span) * n_row + my_row) * rows

    def place(dev):
        return (dev // n_row, lax.rem(dev, n_row))

    def far_first(k, at, count):
        base = jnp.where(at < count // 2, count - 2 - k, k)
        return base + (base >= at).astype(jnp.int32)

    barrier = pltpu.get_barrier_semaphore()

    def greet(k, _):
        pl.semaphore_signal(
            barrier, inc=1, device_id=place(far_first(k, me, n)), device_id_type=MESH
        )
        return 0

    lax.fori_loop(0, n - 1, greet, 0, unroll=4)

    loads = [
        pltpu.make_async_copy(src, dst, local_sem.at[pos])
        for pos, (src, dst) in enumerate(
            [
                (wi_hbm, wi_ref),
                (wl_hbm, wl_ref),
                (ni_hbm, ni_ref),
                (nl_hbm, nl_ref),
                (x_hbm, x_ref),
                (bf_hbm, bf_ref),
                (bs_hbm, bs),
                (bt_hbm, bt),
                (tf_hbm, tf),
                (wp_hbm.at[own], wp),
                (np_hbm.at[own], npj),
                (wt_hbm, wt),
                (nt_hbm, nt),
            ]
        )
    ]
    for load in loads:
        load.start()

    for load in loads[:4]:
        load.wait()
    past = span * n_row * rows // LOW
    slot_at = lax.broadcasted_iota(jnp.int32, (slots, batch), 0)
    spread = (
        lax.rem(lax.broadcasted_iota(jnp.int32, (batch, lanes), 1), batch)
        == lax.broadcasted_iota(jnp.int32, (batch, lanes), 0)
    ).astype(F32).astype(BF16)
    diagonal = (
        lax.broadcasted_iota(jnp.int32, (slots, lanes), 1) // batch
        == lax.broadcasted_iota(jnp.int32, (slots, lanes), 0)
    )
    for t in range(tables):
        for kind, (i_ref, l_ref) in enumerate([(wi_ref, wl_ref), (ni_ref, nl_ref)]):
            ids = i_ref[t]
            high = jnp.where(slot_at < l_ref[t : t + 1, :], ids >> (LOW.bit_length() - 1), past)
            low = ids & (LOW - 1)
            high = jnp.dot(high.astype(F32).astype(BF16), spread, preferred_element_type=F32)
            low = jnp.dot(low.astype(F32).astype(BF16), spread, preferred_element_type=F32)
            row = jnp.sum(jnp.where(diagonal, high * LOW + low, 0.0), axis=0, keepdims=True)
            send_ids[t, kind : kind + 1, :] = row.astype(jnp.int32)

    pl.semaphore_wait(barrier, n - 1)

    def send_one(k, _):
        peer = me ^ jnp.where(k < n // 2, n // 2 + k, k + 1 - n // 2)
        pltpu.make_async_remote_copy(
            src_ref=send_ids.at[peer // n_row // span],
            dst_ref=recv_ids.at[my_row, my_table],
            send_sem=id_send,
            recv_sem=id_recv.at[my_table // n_side, my_row],
            device_id=place(peer),
            device_id_type=MESH,
        ).start()
        return 0

    lax.fori_loop(0, n - 1, send_one, 0, unroll=4)
    pltpu.make_async_copy(
        send_ids.at[own], recv_ids.at[my_row, my_table], id_recv.at[my_table // n_side, my_row]
    ).start()

    for load in loads[4:6]:
        load.wait()
    bottom = dense(x_ref[...], bf_ref[...])
    loads[6].wait()
    bottom = dense(bottom, bs[...])
    loads[7].wait()
    bottom = dense(bottom, bt[...])
    feats[0] = bottom.astype(F32)
    loads[8].wait()
    base = jnp.dot(bottom, tf[0:emb, :], preferred_element_type=F32)
    for load in loads[9:]:
        load.wait()

    high_count = rows // LOW
    high_rows = high_count * batch
    assert high_rows <= 256
    scaled = (npj[...].astype(F32) * (-1.0 / BASE)).astype(BF16)

    @pl.loop(0, rows // PROJECT)
    def _(r):
        at = pl.ds(pl.multiple_of(r * PROJECT, PROJECT), PROJECT)
        flat_wide[:, at] = lax.dot_general(
            wp[...], wt[at, :], (((0,), (1,)), ((), ())), preferred_element_type=F32
        ).astype(BF16)
        flat_narrow[:, at] = lax.dot_general(
            scaled, nt[:, at], (((0,), (0,)), ((), ())), preferred_element_type=F32
        ).astype(BF16)

    at_high = lax.broadcasted_iota(jnp.int32, (high_rows, lanes), 0).astype(F32).astype(BF16)
    at_low = lax.broadcasted_iota(jnp.int32, (LOW, lanes), 0).astype(F32).astype(BF16)
    one, zero = jnp.ones((), BF16), jnp.zeros((), BF16)
    marks = [one, jnp.full((), -BASE, BF16)]
    shift = jnp.full((), 192 * BASE, BF16)
    sample = lax.rem(lax.broadcasted_iota(jnp.int32, (1, lanes), 1), batch)

    my_side = my_table // n_side

    def side_of(step):
        side = SIDES - step if step in (0, 3) else 1 + step
        if step:
            side = jnp.where(side > my_side, side, side - 1)
        else:
            side = my_side
        return jnp.where(my_side == 0, SIDES - 1 - step, side)

    def each(body):
        if n_cc == 1:
            body(0)
        else:
            pl.loop(0, n_cc)(body)

    def taken(row, table):
        ids = recv_ids[row, table] - first_row
        high, low = [], []
        for kind in range(2):
            local = ids[kind : kind + 1, :]
            key = (local >> (LOW.bit_length() - 1)) * batch + sample
            key = jnp.where((key >= 0) & (key < high_rows), key, -1)
            key = key.astype(F32).astype(BF16)
            digit = (local & (LOW - 1)).astype(F32).astype(BF16)
            high.append(jnp.where(key == at_high, marks[kind], zero))
            low.append(jnp.where(digit == at_low, one, zero))
        both = lax.dot_general(
            jnp.concatenate(high, axis=1),
            jnp.concatenate(low, axis=1),
            (((1,), (1,)), ((), ())),
            preferred_element_type=F32,
        ).astype(BF16)
        second = (both + shift) - shift
        return both - second, second

    def count(step, row, cc):
        first_k = side_of(step) * SIDE
        mine = jnp.where(row == my_row, 0, 1)
        for k in range(0, SIDE, 2):
            table = (first_k + k) * n_cc + cc
            at = pl.multiple_of(mine * 2 * SIDE * batch, 2 * SIDE * batch)
            at = pl.ds(at + ((step % 2) * SIDE + k) * batch, 2 * batch)
            found = zip(taken(row, table), taken(row, table + n_cc))
            for kind, (here, there) in enumerate(found):
                for h in range(high_count):
                    own_rows = slice(h * batch, (h + 1) * batch)
                    counts[step // 2, cc, kind, h, at, :] = jnp.concatenate(
                        [here[own_rows], there[own_rows]], axis=0
                    ).astype(F8)

    def weigh(turn, cc):
        given = 2 * SIDE * batch
        for kind, flat in enumerate((flat_wide, flat_narrow)):
            total = jnp.zeros((emb, n_row * given), F32)
            for h in range(high_count):
                total = total + lax.dot_general(
                    flat[:, h * LOW : (h + 1) * LOW],
                    counts[turn, cc, kind, h],
                    (((1,), (1,)), ((), ())),
                    preferred_element_type=F32,
                )
            give[turn, cc, kind] = total[:, :given].astype(BF16)
            keep[turn, cc, kind] = total[:, given:]
        pair_copy(turn, cc).start()

    def pair_copy(step, cc):
        return pltpu.make_async_remote_copy(
            src_ref=give.at[step, cc],
            dst_ref=got.at[step, cc],
            send_sem=pair_send.at[step, cc],
            recv_sem=pair_recv.at[step, cc],
            device_id=(my_table, 1 - my_row),
            device_id_type=MESH,
        )

    def arrive(step, row):
        side = side_of(step)
        arrived = recv_ids.at[row, pl.ds(side * n_side, n_side)]
        pltpu.make_async_copy(arrived, arrived, id_recv.at[side, row]).wait()

    def finish(turn):
        def block(cc):
            pair_copy(turn, cc).wait()
            for kind in range(2):
                total = keep[turn, cc, kind] + got[turn, cc, kind].astype(F32)
                part[turn, cc, :, kind * emb : (kind + 1) * emb] = total.astype(BF16).T
            for half in (1, 0):
                side = side_of(2 * turn + half)
                for k in range(SIDE):
                    peer = (side * SIDE + k) * n_cc + cc
                    at = (half * SIDE + k) * batch
                    pltpu.make_async_remote_copy(
                        src_ref=part.at[turn, cc, pl.ds(at, batch)],
                        dst_ref=recv_part.at[my_table],
                        send_sem=part_send,
                        recv_sem=part_recv,
                        device_id=(peer, 1 - my_row),
                        device_id_type=MESH,
                    ).start()

        each(block)

    for waits, counted, weighed, finished in PLAN:
        for step, row in waits:
            arrive(step, row)

        def block(cc):
            for step, row in counted:
                count(step, row, cc)
            for turn in weighed:
                weigh(turn, cc)

        each(block)
        for turn in finished:
            finish(turn)

    pltpu.make_async_copy(recv_part, recv_part, part_recv).wait()

    for t in range(tables):
        total = recv_part[t * span].astype(F32)
        for s in range(1, span):
            total = total + recv_part[t * span + s].astype(F32)
        total = total.astype(BF16).astype(F32)
        feats[1 + t] = total[:, 0:emb]
        feats[1 + tables + t] = total[:, emb : 2 * emb]

    features = 1 + 2 * tables
    pairs = features * (features - 1) // 2
    column = lax.broadcasted_iota(jnp.int32, (batch, pairs), 1)
    values = jnp.zeros((batch, pairs), F32)
    if features <= 16:
        held = [feats[f] for f in range(features)]
        pos = 0
        for f in range(features):
            for g in range(f + 1, features):
                value = jnp.sum(held[f] * held[g], axis=1, keepdims=True)
                values = jnp.where(column == pos, value, values)
                pos += 1
    else:

        def outer(f, values):
            mine = feats[f]
            start = f * features - f * (f + 1) // 2 - f - 1

            def inner(g, values):
                value = jnp.sum(mine * feats[g], axis=1, keepdims=True)
                return jnp.where(column == start + g, value, values)

            return lax.fori_loop(f + 1, features, inner, values)

        values = lax.fori_loop(0, features - 1, outer, values)
    hidden = base + jnp.dot(
        values.astype(BF16), tf[emb : emb + pairs, :], preferred_element_type=F32
    )
    hidden = jnp.maximum(hidden, 0.0).astype(BF16)
    hid_ref[...] = hidden

    for row in range(n_row):
        left = recv_ids.at[row, pl.ds(0, n_table - (1 if row else 0))]
        pltpu.make_async_copy(left, left, id_send).wait()
    pltpu.make_async_copy(recv_part, recv_part, part_send).wait()


def last_kernel(hid_ref, tl_ref, out_ref, log_ref):
    out_ref[...] = hid_ref[...]
    total = jnp.zeros(log_ref.shape, F32)
    size = tl_ref.shape[1]
    for j in range(tl_ref.shape[0]):
        total = total + lax.dot_general(
            tl_ref[j : j + 1, :],
            hid_ref[:, j * size : (j + 1) * size],
            (((1,), (1,)), ((), ())),
            preferred_element_type=F32,
        )
    log_ref[...] = total


def body(
    dense_input,
    bottom_first,
    bottom_second,
    bottom_third,
    wide_tables,
    narrow_tables,
    wide_indices,
    wide_lengths,
    narrow_indices,
    narrow_lengths,
    wide_projection,
    narrow_projection,
    top_first,
    top_last,
):
    n_table, n_row = lax.axis_size("table"), lax.axis_size("row")
    tables = wide_projection.shape[0]
    span = n_table // tables
    n = n_table * n_row
    batch, slots = dense_input.shape[0], wide_indices.shape[2]
    emb = wide_projection.shape[2]
    rows, width = wide_tables.shape
    top = top_first.shape[1]
    dims = (n_table, n_row, span, tables, batch, slots, emb, rows)
    n_cc = n // CHUNK // n_row
    vmem = pl.BlockSpec(memory_space=pltpu.VMEM)
    hbm = pl.BlockSpec(memory_space=pl.ANY)

    def like(a):
        return pltpu.VMEM(a.shape, a.dtype)

    hidden = pl.pallas_call(
        functools.partial(kernel, dims),
        out_shape=pltpu.VMEM((batch, top), BF16),
        in_specs=[hbm] * 13,
        out_specs=vmem,
        scratch_shapes=[
            like(dense_input),
            like(bottom_first),
            pltpu.VMEM((tables, slots, batch), jnp.int32),
            pltpu.VMEM((tables, batch), jnp.int32),
            pltpu.VMEM((tables, slots, batch), jnp.int32),
            pltpu.VMEM((tables, batch), jnp.int32),
            like(bottom_second),
            like(bottom_third),
            like(wide_tables),
            pltpu.VMEM(narrow_tables.shape[::-1], BF16),
            pltpu.VMEM(wide_projection.shape[1:], BF16),
            pltpu.VMEM(narrow_projection.shape[1:], BF16),
            like(top_first),
            pltpu.VMEM((tables, 2, batch * slots), jnp.int32),
            pltpu.VMEM((n_row, n_table, 2, batch * slots), jnp.int32),
            pltpu.VMEM((2, n_cc, 2, rows // LOW, 2 * SIDE * n_row * batch, LOW), F8),
            pltpu.VMEM((emb, rows), BF16),
            pltpu.VMEM((emb, rows), BF16),
            *[pltpu.VMEM((2, n_cc, 2, emb, 2 * SIDE * batch), d) for d in (BF16, BF16, F32)],
            pltpu.VMEM((2, n_cc, 2 * SIDE * batch, 2 * emb), BF16),
            pltpu.VMEM((n_table, batch, 2 * emb), BF16),
            pltpu.VMEM((1 + 2 * tables, batch, emb), F32),
            pltpu.SemaphoreType.DMA((13,)),
            pltpu.SemaphoreType.DMA,
            pltpu.SemaphoreType.DMA((SIDES, n_row)),
            pltpu.SemaphoreType.DMA,
            pltpu.SemaphoreType.DMA,
            pltpu.SemaphoreType.DMA((2, n_cc)),
            pltpu.SemaphoreType.DMA((2, n_cc)),
        ],
        compiler_params=pltpu.CompilerParams(
            collective_id=0, has_side_effects=True, vmem_limit_bytes=int(60 * 2**20)
        ),
    )(
        dense_input,
        bottom_first,
        bottom_second,
        bottom_third,
        wide_tables,
        narrow_tables.T,
        wide_indices.transpose(1, 2, 0),
        wide_lengths.T,
        narrow_indices.transpose(1, 2, 0),
        narrow_lengths.T,
        wide_projection,
        narrow_projection,
        top_first,
    )
    hidden, logits = pl.pallas_call(
        last_kernel,
        out_shape=(
            jax.ShapeDtypeStruct((batch, top), BF16),
            jax.ShapeDtypeStruct((1, batch), F32),
        ),
        in_specs=[vmem, vmem],
        out_specs=(vmem, vmem),
        compiler_params=pltpu.CompilerParams(vmem_limit_bytes=4 * 2**20),
    )(hidden, top_last.reshape(-1, emb))
    return hidden, logits.reshape(-1)


def solution(mesh):
    split = ("table", "row")
    in_specs = (
        P(split, None),
        P(),
        P(),
        P(),
        P(split, None),
        P(split, None),
        P(split, None, None),
        P(split, None),
        P(split, None, None),
        P(split, None),
        P(),
        P(),
        P(),
        P(),
    )
    out_specs = (P(split, None), P(split))
    return jax.shard_map(body, mesh=mesh, in_specs=in_specs, out_specs=out_specs, check_vma=False)
```

```python
import functools

import jax
import jax.numpy as jnp
from jax import lax
from jax.experimental import pallas as pl
from jax.experimental.pallas import tpu as pltpu
from jax.sharding import PartitionSpec as P

LOW = 256
PROJECT = 1024
BASE = 32
SIDES = 4
SIDE = 4
CHUNK = SIDES * SIDE
PLAN = ((((0, 0), (0, 1)), ((0, 0), (0, 1)), (), ()), (((2, 0), (2, 1)), ((2, 0), (2, 1)), (), ()), (((3, 1),), ((3, 1),), (), ()), (((3, 0),), ((3, 0),), (), ()), ((), (), (1,), ()), (((1, 0), (1, 1)), ((1, 0), (1, 1)), (), ()), ((), (), (), (1,)), ((), (), (0,), ()), ((), (), (), (0,)))
MESH = pl.DeviceIdType.MESH
F32 = jnp.float32
BF16 = jnp.bfloat16
F8 = jnp.float8_e4m3fn


def dense(values, weight):
    return jnp.maximum(jnp.dot(values, weight, preferred_element_type=F32), 0.0).astype(BF16)


def kernel(
    dims,
    x_hbm,
    bf_hbm,
    bs_hbm,
    bt_hbm,
    wt_hbm,
    nt_hbm,
    wi_hbm,
    wl_hbm,
    ni_hbm,
    nl_hbm,
    wp_hbm,
    np_hbm,
    tf_hbm,
    hid_ref,
    x_ref,
    bf_ref,
    wi_ref,
    wl_ref,
    ni_ref,
    nl_ref,
    bs,
    bt,
    wt,
    nt,
    wp,
    npj,
    tf,
    send_ids,
    recv_ids,
    counts,
    flat_wide,
    flat_narrow,
    give,
    got,
    keep,
    part,
    recv_part,
    feats,
    local_sem,
    id_send,
    id_recv,
    part_send,
    part_recv,
    pair_send,
    pair_recv,
):
    n_table, n_row, span, tables, batch, slots, emb, rows = dims
    n = n_table * n_row
    lanes = batch * slots
    n_chunk = n // CHUNK
    n_cc = n_chunk // n_row
    n_side = n_table // SIDES
    owners = span * n_row
    my_table, my_row = lax.axis_index("table"), lax.axis_index("row")
    me = my_table * n_row + my_row
    own = my_table // span
    first_row = (lax.rem(my_table, span) * n_row + my_row) * rows

    def place(dev):
        return (dev // n_row, lax.rem(dev, n_row))

    def far_first(k, at, count):
        base = jnp.where(at < count // 2, count - 2 - k, k)
        return base + (base >= at).astype(jnp.int32)

    barrier = pltpu.get_barrier_semaphore()

    def greet(k, _):
        pl.semaphore_signal(
            barrier, inc=1, device_id=place(far_first(k, me, n)), device_id_type=MESH
        )
        return 0

    lax.fori_loop(0, n - 1, greet, 0, unroll=4)

    loads = [
        pltpu.make_async_copy(src, dst, local_sem.at[pos])
        for pos, (src, dst) in enumerate(
            [
                (wi_hbm, wi_ref),
                (wl_hbm, wl_ref),
                (ni_hbm, ni_ref),
                (nl_hbm, nl_ref),
                (x_hbm, x_ref),
                (bf_hbm, bf_ref),
                (bs_hbm, bs),
                (bt_hbm, bt),
                (tf_hbm, tf),
                (wp_hbm.at[own], wp),
                (np_hbm.at[own], npj),
                (wt_hbm, wt),
                (nt_hbm, nt),
            ]
        )
    ]
    for load in loads:
        load.start()

    for load in loads[:4]:
        load.wait()
    past = span * n_row * rows // LOW
    slot_at = lax.broadcasted_iota(jnp.int32, (slots, batch), 0)
    spread = (
        lax.rem(lax.broadcasted_iota(jnp.int32, (batch, lanes), 1), batch)
        == lax.broadcasted_iota(jnp.int32, (batch, lanes), 0)
    ).astype(F32).astype(BF16)
    diagonal = (
        lax.broadcasted_iota(jnp.int32, (slots, lanes), 1) // batch
        == lax.broadcasted_iota(jnp.int32, (slots, lanes), 0)
    )
    for t in range(tables):
        for kind, (i_ref, l_ref) in enumerate([(wi_ref, wl_ref), (ni_ref, nl_ref)]):
            ids = i_ref[t]
            high = jnp.where(slot_at < l_ref[t : t + 1, :], ids >> (LOW.bit_length() - 1), past)
            low = ids & (LOW - 1)
            high = jnp.dot(high.astype(F32).astype(BF16), spread, preferred_element_type=F32)
            low = jnp.dot(low.astype(F32).astype(BF16), spread, preferred_element_type=F32)
            row = jnp.sum(jnp.where(diagonal, high * LOW + low, 0.0), axis=0, keepdims=True)
            send_ids[t, kind : kind + 1, :] = row.astype(jnp.int32)

    pl.semaphore_wait(barrier, n - 1)

    def send_one(k, _):
        peer = me ^ (n - 1 - k)
        pltpu.make_async_remote_copy(
            src_ref=send_ids.at[peer // n_row // span],
            dst_ref=recv_ids.at[my_row, my_table],
            send_sem=id_send,
            recv_sem=id_recv.at[my_table // n_side, my_row],
            device_id=place(peer),
            device_id_type=MESH,
        ).start()
        return 0

    lax.fori_loop(0, n - 1, send_one, 0, unroll=4)
    pltpu.make_async_copy(
        send_ids.at[own], recv_ids.at[my_row, my_table], id_recv.at[my_table // n_side, my_row]
    ).start()

    for load in loads[4:6]:
        load.wait()
    bottom = dense(x_ref[...], bf_ref[...])
    loads[6].wait()
    bottom = dense(bottom, bs[...])
    loads[7].wait()
    bottom = dense(bottom, bt[...])
    feats[0] = bottom.astype(F32)
    loads[8].wait()
    base = jnp.dot(bottom, tf[0:emb, :], preferred_element_type=F32)
    for load in loads[9:]:
        load.wait()

    high_count = rows // LOW
    high_rows = high_count * batch
    assert high_rows <= 256
    scaled = (npj[...].astype(F32) * (-1.0 / BASE)).astype(BF16)

    @pl.loop(0, rows // PROJECT)
    def _(r):
        at = pl.ds(pl.multiple_of(r * PROJECT, PROJECT), PROJECT)
        flat_wide[:, at] = lax.dot_general(
            wp[...], wt[at, :], (((0,), (1,)), ((), ())), preferred_element_type=F32
        ).astype(BF16)
        flat_narrow[:, at] = lax.dot_general(
            scaled, nt[:, at], (((0,), (0,)), ((), ())), preferred_element_type=F32
        ).astype(BF16)

    at_high = lax.broadcasted_iota(jnp.int32, (high_rows, lanes), 0).astype(F32).astype(BF16)
    at_low = lax.broadcasted_iota(jnp.int32, (LOW, lanes), 0).astype(F32).astype(BF16)
    one, zero = jnp.ones((), BF16), jnp.zeros((), BF16)
    marks = [one, jnp.full((), -BASE, BF16)]
    shift = jnp.full((), 192 * BASE, BF16)
    sample = lax.rem(lax.broadcasted_iota(jnp.int32, (1, lanes), 1), batch)

    my_side = my_table // n_side

    def side_of(step):
        side = SIDES - step if step in (0, 3) else 1 + step
        if step:
            side = jnp.where(side > my_side, side, side - 1)
        else:
            side = my_side
        return jnp.where(my_side == 0, SIDES - 1 - step, side)

    def each(body):
        if n_cc == 1:
            body(0)
        else:
            pl.loop(0, n_cc)(body)

    def taken(row, table):
        ids = recv_ids[row, table] - first_row
        high, low = [], []
        for kind in range(2):
            local = ids[kind : kind + 1, :]
            key = (local >> (LOW.bit_length() - 1)) * batch + sample
            key = jnp.where((key >= 0) & (key < high_rows), key, -1)
            key = key.astype(F32).astype(BF16)
            digit = (local & (LOW - 1)).astype(F32).astype(BF16)
            high.append(jnp.where(key == at_high, marks[kind], zero))
            low.append(jnp.where(digit == at_low, one, zero))
        both = lax.dot_general(
            jnp.concatenate(high, axis=1),
            jnp.concatenate(low, axis=1),
            (((1,), (1,)), ((), ())),
            preferred_element_type=F32,
        ).astype(BF16)
        second = (both + shift) - shift
        return both - second, second

    def count(step, row, cc):
        first_k = side_of(step) * SIDE
        mine = jnp.where(row == my_row, 0, 1)
        for k in range(0, SIDE, 2):
            table = (first_k + k) * n_cc + cc
            at = pl.multiple_of(mine * 2 * SIDE * batch, 2 * SIDE * batch)
            at = pl.ds(at + ((step % 2) * SIDE + k) * batch, 2 * batch)
            found = zip(taken(row, table), taken(row, table + n_cc))
            for kind, (here, there) in enumerate(found):
                for h in range(high_count):
                    own_rows = slice(h * batch, (h + 1) * batch)
                    counts[step // 2, cc, kind, h, at, :] = jnp.concatenate(
                        [here[own_rows], there[own_rows]], axis=0
                    ).astype(F8)

    def weigh(turn, cc):
        given = 2 * SIDE * batch
        for kind, flat in enumerate((flat_wide, flat_narrow)):
            total = jnp.zeros((emb, n_row * given), F32)
            for h in range(high_count):
                total = total + lax.dot_general(
                    flat[:, h * LOW : (h + 1) * LOW],
                    counts[turn, cc, kind, h],
                    (((1,), (1,)), ((), ())),
                    preferred_element_type=F32,
                )
            give[turn, cc, kind] = total[:, :given].astype(BF16)
            keep[turn, cc, kind] = total[:, given:]
        pair_copy(turn, cc).start()

    def pair_copy(step, cc):
        return pltpu.make_async_remote_copy(
            src_ref=give.at[step, cc],
            dst_ref=got.at[step, cc],
            send_sem=pair_send.at[step, cc],
            recv_sem=pair_recv.at[step, cc],
            device_id=(my_table, 1 - my_row),
            device_id_type=MESH,
        )

    def arrive(step, row):
        side = side_of(step)
        arrived = recv_ids.at[row, pl.ds(side * n_side, n_side)]
        pltpu.make_async_copy(arrived, arrived, id_recv.at[side, row]).wait()

    def finish(turn):
        def block(cc):
            pair_copy(turn, cc).wait()
            for kind in range(2):
                total = keep[turn, cc, kind] + got[turn, cc, kind].astype(F32)
                part[turn, cc, :, kind * emb : (kind + 1) * emb] = total.astype(BF16).T
            for half in (1, 0):
                side = side_of(2 * turn + half)
                for k in range(SIDE):
                    peer = (side * SIDE + k) * n_cc + cc
                    at = (half * SIDE + k) * batch
                    pltpu.make_async_remote_copy(
                        src_ref=part.at[turn, cc, pl.ds(at, batch)],
                        dst_ref=recv_part.at[my_table],
                        send_sem=part_send,
                        recv_sem=part_recv,
                        device_id=(peer, 1 - my_row),
                        device_id_type=MESH,
                    ).start()

        each(block)

    for waits, counted, weighed, finished in PLAN:
        for step, row in waits:
            arrive(step, row)

        def block(cc):
            for step, row in counted:
                count(step, row, cc)
            for turn in weighed:
                weigh(turn, cc)

        each(block)
        for turn in finished:
            finish(turn)

    pltpu.make_async_copy(recv_part, recv_part, part_recv).wait()

    for t in range(tables):
        total = recv_part[t * span].astype(F32)
        for s in range(1, span):
            total = total + recv_part[t * span + s].astype(F32)
        total = total.astype(BF16).astype(F32)
        feats[1 + t] = total[:, 0:emb]
        feats[1 + tables + t] = total[:, emb : 2 * emb]

    features = 1 + 2 * tables
    pairs = features * (features - 1) // 2
    column = lax.broadcasted_iota(jnp.int32, (batch, pairs), 1)
    values = jnp.zeros((batch, pairs), F32)
    if features <= 16:
        held = [feats[f] for f in range(features)]
        pos = 0
        for f in range(features):
            for g in range(f + 1, features):
                value = jnp.sum(held[f] * held[g], axis=1, keepdims=True)
                values = jnp.where(column == pos, value, values)
                pos += 1
    else:

        def outer(f, values):
            mine = feats[f]
            start = f * features - f * (f + 1) // 2 - f - 1

            def inner(g, values):
                value = jnp.sum(mine * feats[g], axis=1, keepdims=True)
                return jnp.where(column == start + g, value, values)

            return lax.fori_loop(f + 1, features, inner, values)

        values = lax.fori_loop(0, features - 1, outer, values)
    hidden = base + jnp.dot(
        values.astype(BF16), tf[emb : emb + pairs, :], preferred_element_type=F32
    )
    hidden = jnp.maximum(hidden, 0.0).astype(BF16)
    hid_ref[...] = hidden

    for row in range(n_row):
        left = recv_ids.at[row, pl.ds(0, n_table - (1 if row else 0))]
        pltpu.make_async_copy(left, left, id_send).wait()
    pltpu.make_async_copy(recv_part, recv_part, part_send).wait()


def last_kernel(hid_ref, tl_ref, out_ref, log_ref):
    out_ref[...] = hid_ref[...]
    total = jnp.zeros(log_ref.shape, F32)
    size = tl_ref.shape[1]
    for j in range(tl_ref.shape[0]):
        total = total + lax.dot_general(
            tl_ref[j : j + 1, :],
            hid_ref[:, j * size : (j + 1) * size],
            (((1,), (1,)), ((), ())),
            preferred_element_type=F32,
        )
    log_ref[...] = total


def body(
    dense_input,
    bottom_first,
    bottom_second,
    bottom_third,
    wide_tables,
    narrow_tables,
    wide_indices,
    wide_lengths,
    narrow_indices,
    narrow_lengths,
    wide_projection,
    narrow_projection,
    top_first,
    top_last,
):
    n_table, n_row = lax.axis_size("table"), lax.axis_size("row")
    tables = wide_projection.shape[0]
    span = n_table // tables
    n = n_table * n_row
    batch, slots = dense_input.shape[0], wide_indices.shape[2]
    emb = wide_projection.shape[2]
    rows, width = wide_tables.shape
    top = top_first.shape[1]
    dims = (n_table, n_row, span, tables, batch, slots, emb, rows)
    n_cc = n // CHUNK // n_row
    vmem = pl.BlockSpec(memory_space=pltpu.VMEM)
    hbm = pl.BlockSpec(memory_space=pl.ANY)

    def like(a):
        return pltpu.VMEM(a.shape, a.dtype)

    hidden = pl.pallas_call(
        functools.partial(kernel, dims),
        out_shape=pltpu.VMEM((batch, top), BF16),
        in_specs=[hbm] * 13,
        out_specs=vmem,
        scratch_shapes=[
            like(dense_input),
            like(bottom_first),
            pltpu.VMEM((tables, slots, batch), jnp.int32),
            pltpu.VMEM((tables, batch), jnp.int32),
            pltpu.VMEM((tables, slots, batch), jnp.int32),
            pltpu.VMEM((tables, batch), jnp.int32),
            like(bottom_second),
            like(bottom_third),
            like(wide_tables),
            pltpu.VMEM(narrow_tables.shape[::-1], BF16),
            pltpu.VMEM(wide_projection.shape[1:], BF16),
            pltpu.VMEM(narrow_projection.shape[1:], BF16),
            like(top_first),
            pltpu.VMEM((tables, 2, batch * slots), jnp.int32),
            pltpu.VMEM((n_row, n_table, 2, batch * slots), jnp.int32),
            pltpu.VMEM((2, n_cc, 2, rows // LOW, 2 * SIDE * n_row * batch, LOW), F8),
            pltpu.VMEM((emb, rows), BF16),
            pltpu.VMEM((emb, rows), BF16),
            *[pltpu.VMEM((2, n_cc, 2, emb, 2 * SIDE * batch), d) for d in (BF16, BF16, F32)],
            pltpu.VMEM((2, n_cc, 2 * SIDE * batch, 2 * emb), BF16),
            pltpu.VMEM((n_table, batch, 2 * emb), BF16),
            pltpu.VMEM((1 + 2 * tables, batch, emb), F32),
            pltpu.SemaphoreType.DMA((13,)),
            pltpu.SemaphoreType.DMA,
            pltpu.SemaphoreType.DMA((SIDES, n_row)),
            pltpu.SemaphoreType.DMA,
            pltpu.SemaphoreType.DMA,
            pltpu.SemaphoreType.DMA((2, n_cc)),
            pltpu.SemaphoreType.DMA((2, n_cc)),
        ],
        compiler_params=pltpu.CompilerParams(
            collective_id=0, has_side_effects=True, vmem_limit_bytes=int(60 * 2**20)
        ),
    )(
        dense_input,
        bottom_first,
        bottom_second,
        bottom_third,
        wide_tables,
        narrow_tables.T,
        wide_indices.transpose(1, 2, 0),
        wide_lengths.T,
        narrow_indices.transpose(1, 2, 0),
        narrow_lengths.T,
        wide_projection,
        narrow_projection,
        top_first,
    )
    hidden, logits = pl.pallas_call(
        last_kernel,
        out_shape=(
            jax.ShapeDtypeStruct((batch, top), BF16),
            jax.ShapeDtypeStruct((1, batch), F32),
        ),
        in_specs=[vmem, vmem],
        out_specs=(vmem, vmem),
        compiler_params=pltpu.CompilerParams(vmem_limit_bytes=4 * 2**20),
    )(hidden, top_last.reshape(-1, emb))
    return hidden, logits.reshape(-1)


def solution(mesh):
    split = ("table", "row")
    in_specs = (
        P(split, None),
        P(),
        P(),
        P(),
        P(split, None),
        P(split, None),
        P(split, None, None),
        P(split, None),
        P(split, None, None),
        P(split, None),
        P(),
        P(),
        P(),
        P(),
    )
    out_specs = (P(split, None), P(split))
    return jax.shard_map(body, mesh=mesh, in_specs=in_specs, out_specs=out_specs, check_vma=False)
```
